32 devices in a mesh: rep: 2 (over y), fsdp: 16 (over z, x, core).
Axes of the slice: x: 2, y: 2, z: 4, core: 2. Of those that a mesh axis runs over, the one named last changes fastest.
Arguments:
- tokens: bfloat16 [16384, 4096], P(('rep', 'fsdp')), may hold values from -6 to 6
- value_cot: bfloat16 [16384, 1024], P(('rep', 'fsdp')), may hold values from -6 to 6
- value_weight: bfloat16 [2, 4096, 1024], P('rep', 'fsdp'), may hold values from -0.09375 to 0.09375
- global_params: float32 [2097152], P('fsdp'), may hold values from -6 to 6
- local_params: float32 [2, 2097152], P('rep', 'fsdp'), may hold values from -6 to 6
- momentum: float32 [2097152], P('fsdp'), may hold values from -3 to 3
Outputs:
- token_grad: bfloat16 [16384, 4096], P(('rep', 'fsdp'))
- value_grad: float32 [2, 4096, 1024], P('rep', 'fsdp')
- new_global: float32 [2097152], P('fsdp')
- new_moment: float32 [2097152], P('fsdp')
The draws below stay inside these ranges and needn't reach their ends.
All inputs are finite; a program needn't handle non-finite values.
Results may differ from the reference program's by a relative error of at most 0.001.
Values may be sent and summed in bfloat16 or wider, within the bound.
A program may use at most 128 MiB of HBM per device.

```python
import jax
import jax.numpy as jnp
from jax import lax

D = 4096
KVW = 1024
REPS = 2
GROUP_TOK = 8192
TOKENS = 16384
FRAG = 2097152
N_REP = 2


def spiked(drawn, rng, source, target, shards_of, factor):
    def block_of(dim):
        return (jnp.arange(drawn.shape[dim]) // (drawn.shape[dim] // shards_of)).reshape((-1,) + (1,) * (drawn.ndim - 1 - dim))

    first = jax.random.permutation(rng, shards_of)[block_of(target)]
    far = (block_of(target) + shards_of // 2) % shards_of
    return jnp.where((block_of(source) == first) | (block_of(source) == far), factor * drawn, drawn)


def block_levels(stream_key, extent, shards, smallest, top_value):
    def one(dim, shards_of):
        draws = jax.random.uniform(jax.random.fold_in(jax.random.fold_in(stream_key, 6), dim), (shards_of,), jnp.float32, smallest / len(shards), top_value / len(shards))
        return jnp.repeat(jnp.exp(draws), extent[dim] // shards_of).reshape((-1,) + (1,) * (len(extent) - dim - 1))

    level = one(*shards[0])
    for cut in shards[1:]:
        level = level * one(*cut)
    return level


def noise(key, dims, spread, reach, pieces=(), held_as=jnp.bfloat16):
    drawn = spread * jax.random.normal(key, dims, jnp.float32)
    if pieces:
        drawn = drawn * block_levels(key, dims, pieces, -0.22, 0.18)
    return jnp.clip(drawn, -reach, reach).astype(held_as)


def heavy_noise(stream_key, dims, scale, reach, pieces, heavy, dtype=jnp.bfloat16):
    array = scale * jax.random.normal(stream_key, dims, jnp.float32)
    if pieces:
        array = array * block_levels(stream_key, dims, pieces, -0.22, 0.18)
    return jnp.clip(spiked(array, jax.random.fold_in(stream_key, 3), *heavy), -reach, reach).astype(dtype)


def setup_inputs(seed: int = 0) -> dict:
    keys = jax.random.split(jax.random.key(seed), 7)
    return {
        "tokens": heavy_noise(keys[0], (TOKENS, D), 1.0, 6.0, ((0, 32),), (0, 1, 32, 2.75)),
        "value_cot": noise(keys[1], (TOKENS, KVW), 1.0, 6.0, ((0, 32),)),
        "value_weight": noise(keys[2], (REPS, D, KVW), D ** -0.5, 0.09375, ((0, 2), (1, 16))),
        "global_params": noise(keys[3], (FRAG,), 1.0, 6.0, ((0, 16),), jnp.float32),
        "local_params": noise(keys[4], (REPS, FRAG), 1.0, 6.0, ((0, 2), (1, 16)), jnp.float32),
        "momentum": noise(keys[5], (FRAG,), 0.5, 3.0, ((0, 16),), jnp.float32),
    }


def reference(tokens, value_cot, value_weight, global_params, local_params, momentum):
    token_parts = []
    grad_parts = []
    for replica in range(N_REP):
        inputs = tokens[replica * GROUP_TOK:(replica + 1) * GROUP_TOK]
        cotan = value_cot[replica * GROUP_TOK:(replica + 1) * GROUP_TOK]
        token_parts.append(jnp.dot(cotan, value_weight[replica].T, preferred_element_type=jnp.float32).astype(jnp.bfloat16))
        summed = jnp.dot(inputs.T, cotan, preferred_element_type=jnp.float32)
        grad_parts.append(summed * (1.0 / jnp.sqrt(jnp.float32(GROUP_TOK))))
    token_grad = jnp.concatenate(token_parts, axis=0)
    value_grad = jnp.stack(grad_parts, axis=0)
    pseudo = global_params - lax.optimization_barrier(jnp.sum(local_params, axis=0)) / N_REP
    new_moment = 0.9 * momentum + pseudo
    new_global = global_params - 0.7 * (pseudo + 0.9 * new_moment)
    return (token_grad, value_grad, new_global, new_moment)
```

```python
import functools

import jax
import jax.numpy as jnp
from jax import lax
from jax.experimental import pallas as pl
from jax.experimental.pallas import tpu as pltpu
from jax.sharding import PartitionSpec as P

CORES = 2
COLS = 2
SCALE = 2.0 ** 8


def grad_term(tokens, columns):
    return lax.dot_general(
        tokens, columns, (((0,), (0,)), ((), ())), preferred_element_type=jnp.float32
    )


def acc_cut(extent, tile):
    return extent * 5 // (8 * tile) * tile


def pack(v):
    v = v * SCALE
    v = v * jnp.abs(v)
    return (v * jnp.abs(v)).astype(jnp.bfloat16)


def unpack(p):
    p = p.astype(jnp.float32)
    r = jnp.sqrt(jnp.sqrt(jnp.abs(p))) * (1.0 / SCALE)
    return jnp.where(p < 0, -r, r)


def kernel(groups, reps, factor, x_hbm, c_hbm, w_hbm, g_hbm, l_hbm, m_hbm, tg_ref, vg_ref, ng_ref, nm_ref,
           wbuf, xb, cb, acc_a, acc_b, sax, rax, saz, raz, sbz, rbz, sbx, rbx, gb, lb, mb, lr,
           rw, szr, szl, sx, sc, xl, xs, xrs, cl, cs, own_sem, us, axs, axr, azs, azr, bzs, bzr, bxs):
    nz = groups // (CORES * COLS)
    f = lax.axis_index("fsdp")
    rep = lax.axis_index("rep")
    core, x, z = lax.rem(f, CORES), lax.rem(f // CORES, COLS), f // (CORES * COLS)
    rows, depth = x_hbm.shape[0], w_hbm.shape[0]
    cut = acc_cut(depth, 16)
    wide = acc_cut(c_hbm.shape[1], 128)

    def ident(zz, xx, cc):
        return (zz * COLS + xx) * CORES + cc

    ox, oc = 1 - x, 1 - core
    xdev, cdev = ident(z, ox, core), ident(z, x, oc)
    rdev, ldev = ident(z + 1, x, core), ident(z - 1, x, core)
    has_r, has_l = z < nz - 1, z > 0
    low = z < nz // 2

    def far(i):
        down = nz - 1 - i
        down = jnp.where(down <= z, down - 1, down)
        up = jnp.where(i >= z, i + 1, i)
        return jnp.where(i == nz - 1, z, jnp.where(low, down, up))

    def columns(d):
        return pl.ds(pl.multiple_of(d * depth, depth), depth)

    def xload(q):
        return pltpu.make_async_copy(x_hbm.at[:, columns(q * CORES + core)], xb.at[q, pl.ds(0, rows)], xl.at[q])

    def order(i):
        return jnp.where(i < nz, far(i) * COLS + ox, far(i - nz) * COLS + x)

    nq = nz * COLS
    own = pltpu.make_async_copy(w_hbm, wbuf.at[f], own_sem)
    own.start()
    cload = pltpu.make_async_copy(c_hbm, cb.at[pl.ds(0, rows)], cl)
    cload.start()

    barrier = pltpu.get_barrier_semaphore()

    def greet(dev):
        pl.semaphore_signal(barrier, inc=1, device_id={"fsdp": dev}, device_id_type=pl.DeviceIdType.MESH)

    greet(xdev)
    greet(cdev)
    pl.when(has_r)(lambda: greet(rdev))
    pl.when(has_l)(lambda: greet(ldev))
    pl.semaphore_signal(barrier, inc=1, device_id={"rep": 1 - rep}, device_id_type=pl.DeviceIdType.MESH)

    @pl.loop(0, nq)
    def _(i):
        xload(order(i)).start()

    loads = [pltpu.make_async_copy(src, dst, us.at[n]) for n, (src, dst) in enumerate(((g_hbm, gb), (l_hbm, lb), (m_hbm, mb)))]
    for load in loads:
        load.start()
    pl.semaphore_wait(barrier, 3 + jnp.where(has_r, 1, 0) + jnp.where(has_l, 1, 0))

    def remote(src, dst, ssem, rsem, dev):
        return pltpu.make_async_remote_copy(
            src_ref=src, dst_ref=dst, send_sem=ssem, recv_sem=rsem,
            device_id={"fsdp": dev}, device_id_type=pl.DeviceIdType.MESH)

    def piece(h, blk, ssem, dev):
        part = wbuf.at[blk, pl.ds(0, cut) if h == 0 else pl.ds(cut, depth - cut)]
        return remote(part, part, ssem.at[h, blk], rw.at[h, blk], dev)

    def right(h, blk):
        return piece(h, blk, szr, rdev)

    def left(h, blk):
        return piece(h, blk, szl, ldev)

    def across(h, blk):
        return piece(h, blk, sx, xdev)

    def core_way(h, blk):
        return piece(h, blk, sc, cdev)

    def send_z(h, blk):
        pl.when(has_r)(lambda: right(h, blk).start())
        pl.when(has_l)(lambda: left(h, blk).start())

    def xcopy(q):
        return remote(x_hbm.at[:, columns(q * CORES + oc)], xb.at[q, pl.ds(rows, rows)], xs.at[q], xrs.at[q], cdev)

    cot = remote(c_hbm, cb.at[pl.ds(rows, rows)], cs.at[0], cs.at[1], cdev)
    swap = pltpu.make_async_remote_copy(
        src_ref=l_hbm, dst_ref=lr, send_sem=us.at[3], recv_sem=us.at[4],
        device_id={"rep": 1 - rep}, device_id_type=pl.DeviceIdType.MESH)

    own.wait()
    across(1, f).start()
    send_z(0, f)
    across(0, f).start()
    send_z(1, f)
    cot.start()
    xcopy(order(0)).start()
    core_way(0, f).start()
    core_way(1, f).start()

    @pl.loop(1, nq)
    def _(i):
        xcopy(order(i)).start()

    swap.start()

    def project(d):
        tg_ref[:, columns(d)] = lax.dot_general(
            cb[pl.ds(0, rows)], wbuf[d], (((1,), (1,)), ((), ())), preferred_element_type=jnp.float32
        ).astype(jnp.bfloat16)

    cload.wait()
    project(f)
    core_way(0, cdev).wait_recv()
    core_way(1, cdev).wait_recv()
    project(cdev)
    cot.wait_recv()

    def grad(zz, xx):
        q = zz * COLS + xx
        xload(q).wait()
        xcopy(q).wait_recv()
        return grad_term(xb[q], cb[...])

    def ax(zz):
        return remote(sax.at[zz], rax.at[zz], axs.at[zz], axr.at[zz], xdev)

    other = ident(z, ox, core)

    @pl.loop(0, nz)
    def _(i):
        zz = far(i)
        g = grad(zz, ox)
        sax[zz] = pack(g[:, :wide])
        ax(zz).start()
        acc_b[zz, ox] = g[:, wide:]

        @pl.when(i == 1)
        def _():
            across(1, other).wait_recv()
            send_z(1, other)
            core_way(1, other).start()

    def hop(k, h, xx):
        for ok, zo, fwd, nxt in ((z - k >= 0, z - k, right, has_r), (z + k < nz, z + k, left, has_l)):
            @pl.when(ok)
            def _():
                blk = ident(zo, xx, core)
                fwd(h, blk).wait_recv()
                pl.when(nxt)(lambda: fwd(h, blk).start())
                if h == 0:
                    across(h, blk).start()
                core_way(h, blk).start()

    @pl.loop(0, nz)
    def _(i):
        zz = far(i)
        g = grad(zz, x)
        acc_a[zz] = g[:, :wide]
        acc_b[zz, x] = g[:, wide:]

        @pl.when(i == 1)
        def _():
            hop(1, 0, x)

    def line(acc, sbuf, rbuf, ssem, rsem):
        def copy(way, zz):
            return remote(sbuf.at[zz], rbuf.at[way, zz], ssem.at[zz], rsem.at[way, zz], rdev if way == 0 else ldev)

        def step(s):
            late = nz - 1 - s
            for way, zz, ok, came in ((0, z + late, z <= s, has_l), (1, z - late, nz - 1 - z <= s, has_r)):
                @pl.when(jnp.logical_and(ok, came))
                def _():
                    copy(way, zz).wait_recv()
                    acc[zz] += unpack(rbuf[way, zz])

                if late:
                    @pl.when(ok)
                    def _():
                        sbuf[zz] = pack(acc[zz])
                        copy(way, zz).start()

        def drain():
            for zz in range(nz):
                pl.when(zz > z)(lambda: copy(0, zz).wait_send())
                pl.when(zz < z)(lambda: copy(1, zz).wait_send())

        return step, drain

    step_a, drain_a = line(acc_a, saz, raz, azs, azr)
    step_b, drain_b = line(acc_b, sbz, rbz, bzs, bzr)

    def add_ax(i):
        zz = far(i)
        ax(zz).wait_recv()
        acc_a[zz] += unpack(rax[zz])

    def land(h, d):
        core_way(h, d).wait_recv()

    def column(k):
        for ok, zo in ((z - k >= 0, z - k), (z + k < nz, z + k)):
            @pl.when(ok)
            def _():
                project(ident(zo, x, core))
                d = ident(zo, x, oc)
                land(0, d)
                land(1, d)
                project(d)

    def late(zo):
        blk = ident(zo, ox, core)
        across(0, blk).wait_recv()
        core_way(0, blk).start()
        project(blk)

    def late_other(zo):
        d = ident(zo, ox, oc)
        land(0, d)
        land(1, d)
        project(d)

    step_b(0)
    hop(1, 1, x)
    hop(1, 1, ox)
    add_ax(0)
    step_a(0)
    late(z)
    late_other(z)

    swap.wait_recv()
    for load in loads:
        load.wait()
    pseudo = gb[...] - (lb[...] + lr[...]) / reps
    moment = 0.9 * mb[...] + pseudo
    nm_ref[...] = moment
    ng_ref[...] = gb[...] - 0.7 * (pseudo + 0.9 * moment)

    for s in range(1, nz):
        if s + 1 < nz:
            column(s)
            hop(s + 1, 0, x)
        else:
            column(s)
            late(far(nz - 2))
            if nz > 3:
                late(far(nz - 3))
            late_other(far(nz - 2))
        step_b(s)
        if s + 1 < nz:
            hop(s + 1, 1, x)
            hop(s + 1, 1, ox)
            add_ax(s)
            step_a(s)

    bx = remote(sbx, rbx, bxs.at[0], bxs.at[1], xdev)
    sbx[...] = pack(acc_b[z, ox])
    bx.start()
    if nz > 3:
        late_other(far(nz - 3))
    for i in range(max(nz - 4, 0), -1, -1):
        late(far(i))
        late_other(far(i))
    add_ax(nz - 1)
    step_a(nz - 1)
    vg_ref[:, :wide] = acc_a[z] * factor
    bx.wait_recv()
    vg_ref[:, wide:] = (acc_b[z, x] + unpack(rbx[...])) * factor

    cot.wait_send()
    bx.wait_send()
    swap.wait_send()
    drain_a()
    drain_b()

    @pl.loop(0, nq)
    def _(q):
        xcopy(q).wait_send()
        d = q * CORES + core
        core_way(0, d).wait_send()
        core_way(1, d).wait_send()

    across(1, f).wait_send()

    @pl.loop(0, nz)
    def _(zz):
        ax(zz).wait_send()
        across(0, ident(zz, x, core)).wait_send()
        go_r = jnp.logical_and(zz <= z, has_r)
        go_l = jnp.logical_and(zz >= z, has_l)
        for h, xx in ((0, x), (1, x), (1, ox)):
            pl.when(go_r)(lambda: right(h, ident(zz, xx, core)).wait_send())
            pl.when(go_l)(lambda: left(h, ident(zz, xx, core)).wait_send())


def flush(*refs):
    count = len(refs) // 2
    sems = refs[-1]
    copies = [pltpu.make_async_copy(refs[n], refs[count + n], sems.at[n]) for n in range(count)]
    for copy in copies:
        copy.start()
    for copy in copies:
        copy.wait()


def fused(tokens, value_cot, weight, outer, local, momentum, groups, reps, factor):
    nz = groups // (CORES * COLS)
    rows, wide = tokens.shape[0], value_cot.shape[1]
    depth = weight.shape[0]
    wa = acc_cut(wide, 128)
    wb = wide - wa
    bf, f32 = jnp.bfloat16, jnp.float32
    dma = pltpu.SemaphoreType.DMA
    hbm = pl.BlockSpec(memory_space=pltpu.HBM)
    vmem = pl.BlockSpec(memory_space=pltpu.VMEM)
    frag = outer.shape
    kinds = (((rows, tokens.shape[1]), bf), ((depth, wide), f32), (frag, f32), (frag, f32))
    operands = [pltpu.with_memory_space_constraint(v, pltpu.HBM) for v in (tokens, value_cot, weight, outer, local, momentum)]
    results = pl.pallas_call(
        functools.partial(kernel, groups, reps, factor),
        out_shape=tuple(pltpu.VMEM(shape, kind) for shape, kind in kinds),
        in_specs=[hbm] * 6,
        out_specs=(vmem,) * 4,
        scratch_shapes=[
            pltpu.VMEM((groups, depth, wide), bf),
            pltpu.VMEM((nz * COLS, 2 * rows, depth), bf),
            pltpu.VMEM((2 * rows, wide), bf),
            pltpu.VMEM((nz, depth, wa), f32),
            pltpu.VMEM((nz, COLS, depth, wb), f32),
            pltpu.VMEM((nz, depth, wa), bf),
            pltpu.VMEM((nz, depth, wa), bf),
            pltpu.VMEM((nz, depth, wa), bf),
            pltpu.VMEM((2, nz, depth, wa), bf),
            pltpu.VMEM((nz, COLS, depth, wb), bf),
            pltpu.VMEM((2, nz, COLS, depth, wb), bf),
            pltpu.VMEM((depth, wb), bf),
            pltpu.VMEM((depth, wb), bf),
            pltpu.VMEM(frag, f32), pltpu.VMEM(frag, f32), pltpu.VMEM(frag, f32), pltpu.VMEM(frag, f32),
            dma((2, groups)), dma((2, groups)), dma((2, groups)), dma((2, groups)), dma((2, groups)),
            dma((nz * COLS,)), dma((nz * COLS,)), dma((nz * COLS,)), dma, dma((2,)), dma, dma((5,)),
            dma((nz,)), dma((nz,)), dma((nz,)), dma((2, nz)), dma((nz,)), dma((2, nz)), dma((2,)),
        ],
        compiler_params=pltpu.CompilerParams(
            collective_id=0, has_side_effects=True, vmem_limit_bytes=48 * 1024 * 1024
        ),
        cost_estimate=pl.CostEstimate(flops=80_000_000_000, bytes_accessed=20_000_000, transcendentals=0),
    )(*operands)
    return pl.pallas_call(
        flush,
        out_shape=tuple(pltpu.HBM(shape, kind) for shape, kind in kinds),
        in_specs=[vmem] * 4,
        out_specs=(hbm,) * 4,
        scratch_shapes=[dma((4,))],
        compiler_params=pltpu.CompilerParams(vmem_limit_bytes=1024 * 1024),
        cost_estimate=pl.CostEstimate(flops=1_000_000, bytes_accessed=12_000_000, transcendentals=0),
    )(*[pltpu.with_memory_space_constraint(v, pltpu.VMEM) for v in results])


def shards(tokens, value_cot, value_weight, global_params, local_params, momentum):
    weight = value_weight[0]
    groups = lax.axis_size("fsdp")
    reps = lax.axis_size("rep")
    local = local_params[0]
    factor = 1.0 / float(tokens.shape[0] * groups) ** 0.5
    depth = weight.shape[0]
    if reps == 2 and depth % 128 == 0 and groups % (CORES * COLS) == 0 and groups > CORES * COLS:
        flat = global_params.shape
        tall = (flat[0] // 128, 128)
        token_grad, value_grad, new_global, new_moment = fused(
            tokens, value_cot, weight, global_params.reshape(tall), local.reshape(tall), momentum.reshape(tall),
            groups, reps, factor,
        )
        return (token_grad, value_grad[None], new_global.reshape(flat), new_moment.reshape(flat))
    totals = lax.psum(local, "rep")
    token_grad = lax.dot_general(
        value_cot,
        lax.all_gather(weight, "fsdp", axis=0, tiled=True),
        (((1,), (1,)), ((), ())),
        preferred_element_type=jnp.float32,
    ).astype(jnp.bfloat16)
    value_grad = factor * lax.psum_scatter(
        grad_term(tokens, value_cot), "fsdp", scatter_dimension=0, tiled=True
    )
    pseudo = global_params - totals / reps
    new_moment = 0.9 * momentum + pseudo
    new_global = global_params - 0.7 * (pseudo + 0.9 * new_moment)
    return (token_grad, value_grad[None], new_global, new_moment)


def solution(mesh):
    in_specs = (
        P(("rep", "fsdp"), None),
        P(("rep", "fsdp"), None),
        P("rep", "fsdp", None),
        P("fsdp"),
        P("rep", "fsdp"),
        P("fsdp"),
    )
    out_specs = (P(("rep", "fsdp"), None), P("rep", "fsdp", None), P("fsdp"), P("fsdp"))
    return jax.shard_map(shards, mesh=mesh, in_specs=in_specs, out_specs=out_specs, check_vma=False)
```
